32 devices in a mesh: pool: 2 (over x), dp: 4 (over z), mp: 4 (over y, core).
Axes of the slice: x: 2, y: 2, z: 4, core: 2. Of those that a mesh axis runs over, the one named last changes fastest.
Arguments:
- states: bfloat16 [2, 4, 512, 8192], P('pool', 'dp', 'mp'), may hold values from -8 to 8
- lengths: int32 [2, 4], P(None, 'dp'), may hold values from 128 to 512
- gain: bfloat16 [2, 8192], replicated, may hold values from 0.099609375 to 1.8984375
- w_query: bfloat16 [2, 8192, 4096], P('pool', ('dp', 'mp')), may hold values from -0.088388348 to 0.088388348
- w_keyval: bfloat16 [2, 8192, 1024], P('pool', ('dp', 'mp')), may hold values from -0.088388348 to 0.088388348
Outputs:
- attended: bfloat16 [2, 4, 512, 4096], P('pool', 'dp', None, 'mp')
The draws below stay inside these ranges and needn't reach their ends.
Inputs may be any that keep to these rules, and one draw needn't show every extreme that they name: `lengths`: live positions of each rollout; positions from it on are padding.
All inputs are finite; a program needn't handle non-finite values.
Results may differ from the reference program's by a relative error of at most 0.011.
Values may be sent and summed in bfloat16 or wider, within the bound.
No kernel may reach another device: no remote copies, remote signals or barrier semaphores. Data moves between devices by JAX's collectives and lax.ppermute only.
A program may use at most 128 MiB of HBM per device.

```python
import math
import jax
import jax.numpy as jnp
from jax import lax

D = 8192
HD = 128
QH = 32
KVH = 4
LEN = 512
R = 4


def draw_states(key, part):
    noise = jax.random.normal(jax.random.fold_in(key, 101), (2, R, LEN, D), jnp.float32)
    return jnp.clip(noise, -6.0, 6.0).astype(jnp.bfloat16)


def draw_w_query(key, part):
    scale = D ** (-0.5)
    base = jax.random.normal(jax.random.fold_in(key, 111), (2, D, QH * HD), jnp.float32)
    return (jnp.clip(base, -6.0, 6.0) * scale).astype(jnp.bfloat16)


def draw_w_keyval(key, part):
    scale = D ** (-0.5)
    base = jax.random.normal(jax.random.fold_in(key, 121), (2, D, KVH * 2 * HD), jnp.float32)
    return (jnp.clip(base, -6.0, 6.0) * scale).astype(jnp.bfloat16)


def with_ends(entries, own_key, least, high):
    extent = entries.shape
    index_at = [jax.random.randint(jax.random.fold_in(own_key, axis), (), 0, extent[axis]) for axis in range(len(extent))]
    entries = entries.at[tuple(index_at)].set(least)
    longest = extent.index(max(extent))
    index_at[longest] = (index_at[longest] + 1) % extent[longest]
    return entries.at[tuple(index_at)].set(high)


def setup_inputs(seed: int = 0) -> dict:
    seeds = jax.random.split(jax.random.key(seed), 6)
    states = draw_states(jax.random.fold_in(seeds[5], 71), 0)
    lengths = with_ends(jax.random.randint(seeds[1], (2, R), LEN // 4, LEN + 1), jax.random.fold_in(seeds[1], 1), LEN // 4, LEN).astype(jnp.int32)
    gain = jnp.clip(1.0 + 0.18 * jax.random.normal(seeds[2], (2, D), jnp.float32), 0.099609375, 1.8984375).astype(jnp.bfloat16)
    w_query = draw_w_query(jax.random.fold_in(seeds[5], 71), 0)
    w_keyval = draw_w_keyval(jax.random.fold_in(seeds[5], 71), 0)
    return dict(states=states, lengths=lengths, gain=gain, w_query=w_query, w_keyval=w_keyval)


def rollout_attention(normed, w_query, w_keyval, length):
    query = jnp.dot(normed, w_query, preferred_element_type=jnp.float32).astype(jnp.bfloat16)
    keyval = jnp.dot(normed, w_keyval, preferred_element_type=jnp.float32).astype(jnp.bfloat16)
    keyval = keyval.reshape(LEN, KVH, 2 * HD)
    keys = keyval[:, :, :HD].astype(jnp.float32)
    values = keyval[:, :, HD:].astype(jnp.float32)
    grouped = query.reshape(LEN, KVH, QH // KVH, HD).astype(jnp.float32)
    scores = jnp.einsum('tkgd,skd->kgts', grouped, keys) / math.sqrt(HD)
    places = jnp.arange(LEN, dtype=jnp.int32)
    allowed = (places[None, :] <= places[:, None]) & (places[None, :] < length)
    scores = jnp.where(allowed, scores, jnp.float32(-1e+30))
    peak = lax.optimization_barrier(jnp.max(scores, axis=-1, keepdims=True))
    expo = jnp.exp(scores - peak)
    probs = (expo / lax.optimization_barrier(jnp.sum(expo, axis=-1, keepdims=True))).astype(jnp.bfloat16)
    result = jnp.einsum('kgts,skd->tkgd', probs.astype(jnp.float32), values)
    result = result.reshape(LEN, QH * HD) * (places < length).astype(jnp.float32)[:, None]
    return result.astype(jnp.bfloat16)

def reference(states, lengths, gain, w_query, w_keyval):
    results = []
    for train in range(2):
        source = 1 - train
        rows = states[source].astype(jnp.float32)
        meansq = lax.optimization_barrier(jnp.mean(rows * rows, axis=-1, keepdims=True))
        normed = (rows * lax.rsqrt(meansq + 1e-05) * gain[source].astype(jnp.float32)).astype(jnp.bfloat16)

        def one(item):
            return rollout_attention(item[0], w_query[source], w_keyval[source], item[1])
        results.append(lax.map(one, (normed, lengths[source])))
    return jnp.stack(results)
```

```python
import functools
import math

import jax
import jax.numpy as jnp
from jax import lax
from jax.experimental import pallas as pl
from jax.experimental.pallas import tpu as pltpu
from jax.sharding import PartitionSpec as P

HD = 128
QH = 32
KVH = 4
F32 = jnp.float32
BF16 = jnp.bfloat16


def xor_pairs(size, bits):
    return [(i, i ^ bits) for i in range(size)]


def swap(value, axis, bits):
    return lax.ppermute(value, axis, xor_pairs(lax.axis_size(axis), bits))


def normalize(rows, gain_row):
    values = rows.astype(F32)
    meansq = jnp.mean(values * values, axis=-1, keepdims=True)
    return (values * lax.rsqrt(meansq + 1e-05) * gain_row.astype(F32)).astype(BF16)


def matmul_kernel(count, me_ref, *refs):
    a_refs, w_refs = refs[:count], refs[count : 2 * count]
    o_ref, a_all = refs[2 * count], refs[2 * count + 1]
    me = me_ref[0]
    rows = a_refs[0].shape[0]
    depth = w_refs[0].shape[0]
    width = w_refs[0].shape[1]
    for r in range(count):
        for j in range(count):
            at = pl.multiple_of((me ^ j) * depth, depth)
            a_all[r * rows : (r + 1) * rows, j * depth : (j + 1) * depth] = a_refs[r][:, pl.ds(at, depth)]
    for n in range(width // HD):
        cols = slice(n * HD, (n + 1) * HD)
        total = None
        for j in range(count):
            part = jnp.dot(
                a_all[:, j * depth : (j + 1) * depth], w_refs[j][:, cols], preferred_element_type=F32
            )
            total = part if total is None else total + part
        o_ref[:, cols] = total


def matmul(me, a_blocks, w_blocks):
    count = len(a_blocks)
    rows, depth = a_blocks[0].shape
    width = w_blocks[0].shape[1]
    vmem = pl.BlockSpec(memory_space=pltpu.VMEM)
    return pl.pallas_call(
        functools.partial(matmul_kernel, count),
        out_shape=jax.ShapeDtypeStruct((count * rows, width), F32),
        in_specs=[pl.BlockSpec(memory_space=pltpu.SMEM)] + [vmem] * (2 * count),
        out_specs=vmem,
        scratch_shapes=[pltpu.VMEM((count * rows, depth), BF16)],
        cost_estimate=pl.CostEstimate(
            flops=2 * count * rows * depth * width,
            bytes_accessed=2 * count * rows * depth + 2 * depth * width + 4 * count * rows * width,
            transcendentals=0,
        ),
        name="project",
    )(me, *a_blocks, *w_blocks)


def attend_kernel(count, scalars, q_ref, k_ref, v_ref, o_ref):
    me, length = scalars[0], scalars[1]
    seqlen = k_ref.shape[0]
    block = seqlen // count
    heads = q_ref.shape[1] // HD

    def places(axis, shape):
        index = lax.broadcasted_iota(jnp.int32, shape, axis)
        return ((index // block) ^ me) * block + index % block

    keys, values = k_ref[...], v_ref[...]
    for b in range(count):
        own = places_of = b ^ me
        start = pl.multiple_of(own * block, block)
        qplaces = start + lax.broadcasted_iota(jnp.int32, (block, seqlen), 0)
        kplaces = places(1, (block, seqlen))
        allowed = (kplaces <= qplaces) & (kplaces < length)
        live = (start + lax.broadcasted_iota(jnp.int32, (block, HD), 0)) < length
        for h in range(heads):
            cols = slice(h * HD, (h + 1) * HD)
            scores = lax.dot_general(
                q_ref[b * block : (b + 1) * block, cols], keys, (((1,), (1,)), ((), ())),
                preferred_element_type=F32,
            ) * (1.0 / math.sqrt(HD))
            scores = jnp.where(allowed, scores, jnp.float32(-1e30))
            expo = jnp.exp(scores - jnp.max(scores, axis=-1, keepdims=True))
            probs = (expo / jnp.sum(expo, axis=-1, keepdims=True)).astype(BF16)
            result = jnp.dot(probs, values, preferred_element_type=F32)
            o_ref[pl.ds(start, block), cols] = jnp.where(live, result, 0.0).astype(BF16)


def attend(count, scalars, query, keys, values):
    seqlen, width = query.shape
    vmem = pl.BlockSpec(memory_space=pltpu.VMEM)
    return pl.pallas_call(
        functools.partial(attend_kernel, count),
        out_shape=jax.ShapeDtypeStruct((seqlen, width), BF16),
        in_specs=[pl.BlockSpec(memory_space=pltpu.SMEM)] + [vmem] * 3,
        out_specs=vmem,
        cost_estimate=pl.CostEstimate(
            flops=4 * seqlen * seqlen * width,
            bytes_accessed=4 * seqlen * width + 4 * seqlen * HD,
            transcendentals=seqlen * seqlen * (width // HD),
        ),
        name="attend",
    )(scalars, query, keys, values)


def split_heads(heads):
    parts = []
    while heads:
        take = min(3 if len(parts) in (1, 2) else 1, heads)
        parts.append(take)
        heads -= take
    return parts


def partial_plan(states, lengths, gain, w_query, w_keyval):
    own = lax.axis_index("pool")
    other = 1 - own
    n = lax.axis_size("dp")
    count = lax.axis_size("mp")
    z = lax.axis_index("dp")
    me = lax.axis_index("mp")
    me_array = me[None].astype(jnp.int32)
    rows = states.shape[2]
    width = states.shape[3]
    depth = width // n
    q_width = w_query.shape[2] // count
    kv_width = w_keyval.shape[2] // count
    kv_heads = kv_width // (2 * HD)
    q_per_kv = q_width // HD // kv_heads

    groups = []
    for heads in split_heads(q_width // HD):
        first = groups[-1][1] if groups else 0
        groups.append((first, first + heads))

    def columns(g, target):
        lo, hi = groups[g]
        q = lax.dynamic_slice(w_query[0], (0, target * q_width + lo * HD), (w_query.shape[1], (hi - lo) * HD))
        if g:
            return q
        kv = lax.dynamic_slice(w_keyval[0], (0, target * kv_width), (w_keyval.shape[1], kv_width))
        return jnp.concatenate([kv, q], axis=1)

    weights = []
    for g in range(len(groups)):
        blocks = [columns(g, me)]
        for s in range(1, count):
            with jax.named_scope(f"w{g}_{s}"):
                blocks.append(swap(columns(g, me ^ s), "mp", s))
        weights.append(blocks)

    normed = normalize(states[0, 0], lax.dynamic_index_in_dim(gain, own, 0, keepdims=False))
    tokens = {}
    for s in reversed(range(n)):
        piece = lax.dynamic_slice(normed, (0, (z ^ s) * depth), (rows, depth))
        if s:
            with jax.named_scope(f"az{s}"):
                piece = swap(piece, "dp", s)
        blocks = {0: piece}
        bit = count // 2
        while bit:
            for have in list(blocks):
                with jax.named_scope(f"am{s}_{bit}_{have}"):
                    blocks[have | bit] = swap(blocks[have], "mp", bit)
            bit //= 2
        tokens[s] = [blocks[j] for j in range(count)]

    pairs = lambda step, d: [(i, i + step) for i in range(n) if 0 <= i + step * d < n]
    across = lambda step: [
        (x * n + i, (1 - x) * n + i + step) for x in range(2) for i in range(n) if 0 <= i + step < n
    ]
    results = []
    live = lax.dynamic_index_in_dim(lengths, other, 0, keepdims=False)
    scalars = jnp.stack([me.astype(jnp.int32), live[0]])
    keyval = None
    for g, (lo, hi) in enumerate(groups):
        sums = {s: matmul(me_array, tokens[s], weights[g]) for s in reversed(range(n))}

        def towards(step, d):
            sources = sorted({i ^ (i + step * d) for i in range(n) if 0 <= i + step * d < n})
            pick = z ^ (z + step * d)
            value = sums[sources[0]]
            for s in sources[1:]:
                value = jnp.where(pick == s, sums[s], value)
            return value

        arrived = []
        for step in (1, -1):
            carry = None
            for d in range(n - 1, 0, -1):
                value = towards(step, d)
                if carry is not None:
                    value = value + carry.astype(F32)
                value = value.astype(BF16)
                with jax.named_scope(f"c{g}_{'l' if step < 0 else 'r'}{d}"):
                    if d > 1:
                        carry = lax.ppermute(value, "dp", pairs(step, d))
                    else:
                        carry = lax.ppermute(value, ("pool", "dp"), across(step))
            arrived.append(carry)
        with jax.named_scope(f"c{g}_own"):
            arrived.append(swap(sums[0].astype(BF16), "pool", 1))
        total = sum(part.astype(F32) for part in arrived).astype(BF16)
        if g == 0:
            keyval, total = total[:, :kv_width], total[:, kv_width:]
        head = lo
        while head < hi:
            kv = head // q_per_kv
            last = min(hi, (kv + 1) * q_per_kv)
            results.append(
                attend(
                    count,
                    scalars,
                    total[:, (head - lo) * HD : (last - lo) * HD],
                    keyval[:, 2 * kv * HD : (2 * kv + 1) * HD],
                    keyval[:, (2 * kv + 1) * HD : (2 * kv + 2) * HD],
                )
            )
            head = last
    return jnp.concatenate(results, axis=1)[None, None]


def gather_plan(states, lengths, gain, w_query, w_keyval):
    own = lax.axis_index("pool")
    count = lax.axis_size("mp")
    normed = normalize(states, lax.dynamic_index_in_dim(gain, own, 0, keepdims=False))
    whole = lax.all_gather(normed, "mp", axis=2, tiled=True)
    tokens = whole[0, 0]
    moved = [
        lax.all_gather(
            lax.all_to_all(w[0], "mp", split_axis=1, concat_axis=0, tiled=True), "dp", axis=0, tiled=True
        )
        for w in (w_query, w_keyval)
    ]
    query, keyval = (
        jnp.dot(tokens, w, preferred_element_type=F32).astype(BF16) for w in moved
    )
    live = lax.dynamic_index_in_dim(lengths, own, 0, keepdims=False)
    scalars = jnp.stack([jnp.int32(0), live[0]])
    per = QH // KVH * HD
    results = [
        attend(
            count,
            scalars,
            query[:, kv * per : (kv + 1) * per],
            keyval[:, 2 * kv * HD : (2 * kv + 1) * HD],
            keyval[:, (2 * kv + 1) * HD : (2 * kv + 2) * HD],
        )
        for kv in range(keyval.shape[1] // (2 * HD))
    ]
    return swap(jnp.concatenate(results, axis=1), "pool", 1)[None, None]


def on_device(states, lengths, gain, w_query, w_keyval):
    n = lax.axis_size("dp")
    seqlen = states.shape[2] * lax.axis_size("mp")
    depth = states.shape[3] // n
    width = w_query.shape[2] + w_keyval.shape[2]
    if seqlen * (depth + width) < depth * width:
        return partial_plan(states, lengths, gain, w_query, w_keyval)
    return gather_plan(states, lengths, gain, w_query, w_keyval)


def solution(mesh):
    in_specs = (
        P("pool", "dp", "mp", None),
        P(None, "dp"),
        P(),
        P("pool", ("dp", "mp"), None),
        P("pool", ("dp", "mp"), None),
    )
    out_specs = P("pool", "dp", None, "mp")
    return jax.shard_map(
        on_device, mesh=mesh, in_specs=in_specs, out_specs=out_specs, check_vma=False
    )
```

```python
import functools
import math

import jax
import jax.numpy as jnp
from jax import lax
from jax.experimental import pallas as pl
from jax.experimental.pallas import tpu as pltpu
from jax.sharding import PartitionSpec as P

HD = 128
F32 = jnp.float32
BF16 = jnp.bfloat16


def swap(value, axis, bits):
    return lax.ppermute(value, axis, [(i, i ^ bits) for i in range(lax.axis_size(axis))])


def normalize(rows, gain_row):
    values = rows.astype(F32)
    meansq = jnp.mean(values * values, axis=-1, keepdims=True)
    return (values * lax.rsqrt(meansq + 1e-05) * gain_row.astype(F32)).astype(BF16)


SMEM = pl.BlockSpec(memory_space=pltpu.SMEM)
NEAR = pl.BlockSpec(memory_space=pltpu.VMEM)
ANY = pl.BlockSpec(memory_space=pl.ANY)
ALONE = pltpu.CompilerParams(vmem_limit_bytes=62 << 20)


def whole(shape):
    return pl.BlockSpec(shape, lambda i: (0,) * len(shape))


def limit(held):
    return pltpu.CompilerParams(vmem_limit_bytes=held + (2 << 20))


def cost(flops, moved, exps=0):
    return pl.CostEstimate(flops=flops, bytes_accessed=moved, transcendentals=exps)


def columns_copies(target, span, kv_width, q_width, w_query, w_keyval, out, sems):
    copies, at = [], 0
    if span.start < kv_width:
        at = kv_width - span.start
        cols = pl.ds(pl.multiple_of(target * kv_width + span.start, HD), at)
        copies.append(pltpu.make_async_copy(w_keyval.at[:, cols], out.at[:, :at], sems.at[0]))
    lo, width = max(span.start, kv_width) - kv_width, span.stop - span.start
    cols = pl.ds(pl.multiple_of(target * q_width + lo, HD), width - at)
    copies.append(pltpu.make_async_copy(w_query.at[:, cols], out.at[:, at:], sems.at[1]))
    return copies


class Cuts:
    def __init__(self, wanted, widths, depth):
        self.wanted, self.widths = wanted, widths
        shapes = [(depth, span.stop - span.start) for _, span in wanted]
        self.out_shape = [jax.ShapeDtypeStruct(shape, BF16) for shape in shapes]
        self.scratch = [pltpu.VMEM(shape, BF16) for shape in shapes]
        self.scratch += [pltpu.SemaphoreType.DMA((len(wanted), 2)), pltpu.SemaphoreType.DMA((len(wanted),))]
        self.moved = sum(4 * rows * cols for rows, cols in shapes)

    def start(self, w_query, w_keyval, outs, scratch):
        me = lax.axis_index("mp")
        held, sems, out_sems = scratch[:-2], scratch[-2], scratch[-1]
        self.inward = [
            columns_copies(me ^ bits, span, *self.widths, w_query, w_keyval, held[i], sems.at[i])
            for i, (bits, span) in enumerate(self.wanted)
        ]
        self.outward = [pltpu.make_async_copy(held[i], outs[i], out_sems.at[i]) for i in range(len(outs))]
        for copies in self.inward:
            for copy in copies:
                copy.start()

    def pass_on(self):
        for copies, out in zip(self.inward, self.outward):
            for copy in copies:
                copy.wait()
            out.start()

    def finish(self):
        for out in self.outward:
            out.wait()


def cut_kernel(cuts, w_query, w_keyval, *refs):
    count = len(cuts.wanted)
    cuts.start(w_query, w_keyval, refs[:count], refs[count:])
    cuts.pass_on()
    cuts.finish()


def cut(cuts, w_query, w_keyval):
    return pl.pallas_call(
        functools.partial(cut_kernel, cuts),
        out_shape=cuts.out_shape,
        in_specs=[ANY, ANY],
        out_specs=[ANY] * len(cuts.wanted),
        scratch_shapes=cuts.scratch,
        compiler_params=ALONE,
        cost_estimate=cost(0, cuts.moved),
        name="cut",
    )(w_query, w_keyval)


def stack_kernel(spans, *refs):
    me = lax.axis_index("mp")
    blocks, o_ref, sems = refs[:-2], refs[-2], refs[-1]
    copies = []
    for r, (ref, span) in enumerate(zip(blocks, spans)):
        depth = ref.shape[0]
        rows = pl.ds(pl.multiple_of((me ^ r) * depth, depth), depth)
        copies.append(pltpu.make_async_copy(ref.at[:, span], o_ref.at[rows, :], sems.at[r]))
    for copy in copies:
        copy.start()
    for copy in copies:
        copy.wait()


def stack_rows(span, shared, blocks):
    depth = shared[0].shape[0]
    width = span.stop - span.start
    spans = [span] * len(shared) + [slice(0, width)] * len(blocks)
    shape = (depth * len(spans), width)
    return pl.pallas_call(
        functools.partial(stack_kernel, spans),
        out_shape=jax.ShapeDtypeStruct(shape, BF16),
        in_specs=[ANY] * len(spans),
        out_specs=NEAR,
        scratch_shapes=[pltpu.SemaphoreType.DMA((len(spans),))],
        compiler_params=limit(2 * shape[0] * width),
        cost_estimate=cost(0, 4 * shape[0] * width),
        name="stack",
    )(*shared, *blocks)


def begin_kernel(chunk, n, cuts, x_ref, gain_ref, w_query, w_keyval, *refs):
    count = len(cuts.wanted)
    outs, cut_outs, refs = refs[:n], refs[n : n + count], refs[n + count :]
    x_held, gain_held, scaled, sems, gain_sem, out_sems = refs[:6]
    own, z = lax.axis_index("pool"), lax.axis_index("dp")
    depth = outs[0].shape[1]
    pieces = [slice(at, at + chunk) for at in range(0, x_ref.shape[0], chunk)]
    copies = [pltpu.make_async_copy(x_ref.at[rows, :], x_held.at[rows, :], sems.at[i]) for i, rows in enumerate(pieces)]
    gain_copy = pltpu.make_async_copy(gain_ref, gain_held, gain_sem)
    copies[0].start()
    gain_copy.start()
    for copy in copies[1:]:
        copy.start()
    cuts.start(w_query, w_keyval, cut_outs, refs[6:])
    gain_copy.wait()
    gain_row = jnp.where(own == 0, gain_held[0:1, :].astype(F32), gain_held[1:2, :].astype(F32))
    outward = []
    for i, rows in enumerate(pieces):
        copies[i].wait()
        values = x_held[rows, :].astype(F32)
        meansq = jnp.mean(values * values, axis=-1, keepdims=True)
        scaled[rows, :] = (values * lax.rsqrt(meansq + 1e-05) * gain_row).astype(BF16)
        for s, o_ref in enumerate(outs):
            cols = pl.ds(pl.multiple_of((z ^ s) * depth, depth), depth)
            out = pltpu.make_async_copy(scaled.at[rows, cols], o_ref.at[rows, :], out_sems.at[i, s])
            out.start()
            outward.append(out)
        if i == len(pieces) // 2:
            cuts.pass_on()
    for out in outward:
        out.wait()
    cuts.finish()


def begin(rows, gain, w_query, w_keyval, n, cuts):
    count, width = rows.shape
    chunk = min(16, count)
    outs = pl.pallas_call(
        functools.partial(begin_kernel, chunk, n, cuts),
        out_shape=[jax.ShapeDtypeStruct((count, width // n), BF16)] * n + cuts.out_shape,
        in_specs=[ANY] * 4,
        out_specs=[ANY] * (n + len(cuts.wanted)),
        scratch_shapes=[
            pltpu.VMEM(rows.shape, BF16),
            pltpu.VMEM(gain.shape, BF16),
            pltpu.VMEM(rows.shape, BF16),
            pltpu.SemaphoreType.DMA((count // chunk,)),
            pltpu.SemaphoreType.DMA,
            pltpu.SemaphoreType.DMA((count // chunk, n)),
        ]
        + cuts.scratch,
        compiler_params=ALONE,
        cost_estimate=cost(4 * count * width, 4 * count * width + cuts.moved),
        name="begin",
    )(rows, gain, w_query, w_keyval)
    return outs[:n], outs[n:]


def project_kernel(sizes, added, *refs):
    count = sum(sizes)
    blocks, w_ref, more, refs = refs[:count], refs[count], refs[count + 1 :][: len(added)], refs[count + 1 + len(added) :]
    o_ref = refs[0]
    seqlen = o_ref.shape[0] // len(sizes)
    z = lax.axis_index("dp")
    middle = (z == 1) | (z == 2)
    for t, size in enumerate(sizes):
        mine, blocks = blocks[:size], blocks[size:]
        if size == 1:
            tokens = mine[0][...]
        else:
            rows = mine[0].shape[0]
            for i, ref in enumerate(mine):
                refs[1][i * rows : (i + 1) * rows, :] = ref[...]
            tokens = refs[1][...]
        total = jnp.dot(tokens, w_ref[...], preferred_element_type=F32)
        for ref, (start, masked) in zip(more, added):
            part = ref[start + t * seqlen : start + (t + 1) * seqlen, :].astype(F32)
            total = total + (jnp.where(middle, part, 0.0) if masked else part)
        o_ref[t * seqlen : (t + 1) * seqlen, :] = total.astype(BF16)


def project(tokens, weights, added=()):
    join = isinstance(tokens[0], list)
    groups = tokens if join else [[array] for array in tokens]
    depth, width = weights.shape
    seqlen = sum(block.shape[0] for block in groups[0])
    flat = [block for group in groups for block in group]
    rows = seqlen * len(groups)
    out_shape = [jax.ShapeDtypeStruct((rows, width), BF16)]
    if join:
        out_shape.append(jax.ShapeDtypeStruct((seqlen, depth), BF16))
    out = pl.pallas_call(
        functools.partial(
            project_kernel, [len(group) for group in groups], [(start, masked) for _, start, masked in added]
        ),
        out_shape=out_shape,
        in_specs=[NEAR] * (len(flat) + 1 + len(added)),
        out_specs=[NEAR] * len(out_shape),
        compiler_params=limit(4 << 20),
        cost_estimate=cost(2 * rows * depth * width, 2 * rows * depth + 2 * depth * width + 2 * rows * width),
        name="project",
    )(*flat, weights, *[array for array, _, _ in added])
    return out if join else out[0]


def attend_kernel(count, heads, skip, scalars, q_ref, kv_ref, o_ref, keys, values):
    me, length = scalars[0], scalars[1]
    seqlen = keys.shape[0]
    block = seqlen // count
    starts = [pl.multiple_of((b ^ me) * block, block) for b in range(count)]
    for b in range(count):
        keys[b * block : (b + 1) * block, :] = kv_ref[pl.ds(starts[b], block), :HD]
        values[b * block : (b + 1) * block, :] = kv_ref[pl.ds(starts[b], block), HD : 2 * HD]
    for b in range(count):
        reach = (b + 1) * block
        query = jnp.concatenate(
            [q_ref[pl.ds(starts[b], block), skip + h * HD : skip + (h + 1) * HD] for h in range(heads)], axis=0
        )
        scores = lax.dot_general(
            query, keys[:reach, :], (((1,), (1,)), ((), ())), preferred_element_type=F32
        ) * (1.0 / math.sqrt(HD))
        places = b * block + lax.rem(lax.broadcasted_iota(jnp.int32, (heads * block, 1), 0), block)
        last = jnp.minimum(places, length - 1)
        allowed = lax.broadcasted_iota(jnp.int32, (heads * block, reach), 1) <= last
        scores = jnp.where(allowed, scores, jnp.float32(-1e30))
        expo = jnp.exp(scores - jnp.max(scores, axis=-1, keepdims=True))
        probs = (expo * (1.0 / jnp.sum(expo, axis=-1, keepdims=True))).astype(BF16)
        result = jnp.dot(probs, values[:reach, :], preferred_element_type=F32)
        result = jnp.where(places < length, result, 0.0).astype(BF16)
        for h in range(heads):
            o_ref[b * block : reach, h * HD : (h + 1) * HD] = result[h * block : (h + 1) * block]


def attend(count, scalars, query, skip, heads, keyval):
    seqlen = keyval.shape[0]
    return pl.pallas_call(
        functools.partial(attend_kernel, count, heads, skip),
        out_shape=jax.ShapeDtypeStruct((seqlen, heads * HD), BF16),
        grid=(1,),
        in_specs=[SMEM, whole(query.shape), pl.BlockSpec((seqlen, 2 * HD), lambda i: (0, 0))],
        out_specs=whole((seqlen, heads * HD)),
        scratch_shapes=[pltpu.VMEM((seqlen, HD), BF16)] * 2,
        cost_estimate=cost(4 * seqlen * seqlen * HD * heads, 4 * seqlen * HD * heads, seqlen * seqlen * heads),
        compiler_params=limit(12 * seqlen * (query.shape[1] + seqlen * heads)),
        name="attend",
    )(scalars, query, keyval)


GROUP_HEADS = (2, 2, 2, 2)


def line_plan(states, lengths, gain, w_query, w_keyval):
    own = lax.axis_index("pool")
    n = lax.axis_size("dp")
    count = lax.axis_size("mp")
    me = lax.axis_index("mp")
    q_width = w_query.shape[2] // count
    kv_width = w_keyval.shape[2] // count
    w_query, w_keyval = w_query[0], w_keyval[0]

    spans, at = [], 0
    for g, heads in enumerate(GROUP_HEADS):
        to = at + heads * HD + (0 if g else kv_width)
        spans.append(slice(at, to))
        at = to

    widths = (kv_width, q_width)
    far = list(range(2, count))
    first = Cuts([(s, spans[0]) for s in far], widths, w_query.shape[0])
    normed, sent = begin(states[0, 0], gain, w_query, w_keyval, n, first)
    wanted = [(s, span) for span in spans[1:] for s in far] + [(bits, slice(0, at)) for bits in (0, 1)]
    *rest, mine, near = cut(Cuts(wanted, widths, w_query.shape[0]), w_query, w_keyval)
    sent = list(sent) + rest
    received = [[swap(sent[g * len(far) + i], "mp", s) for i, s in enumerate(far)] for g in range(len(spans))]
    near = swap(near, "mp", 1)
    weights = []
    for g, span in enumerate(spans):
        weights.append(stack_rows(span, [mine, near], received[g]))

    tokens = {}
    for s in range(n):
        piece = normed[s]
        if s:
            piece = swap(piece, "dp", s)
        blocks = {0: piece}
        bit = count // 2
        while bit:
            for have in list(blocks):
                blocks[have | bit] = swap(blocks[have], "mp", bit)
            bit //= 2
        tokens[s] = [blocks[j] for j in range(count)]

    def outer(value):
        return swap(value, "dp", 1)

    def inward(value, pairs=((0, 1), (3, 2))):
        return lax.ppermute(value, "dp", pairs)

    def inner(value):
        pairs = [(x * n + i, x * n + 3 - i) for x in range(2) for i in (1, 2)]
        pairs += [(x * n + i, (1 - x) * n + i) for x in range(2) for i in (0, 3)]
        return lax.ppermute(value, ("pool", "dp"), pairs)

    live = lax.dynamic_index_in_dim(lengths, own, 0, keepdims=False)
    scalars = jnp.stack([me.astype(jnp.int32), live[0]])
    seqlen = count * states.shape[2]
    pieces = []
    keyval = None
    for g, w in enumerate(weights):
        if g == 0:
            value, tokens[1] = project([tokens[1]], w)
            a1 = inward(value)
            value, tokens[3] = project([tokens[3]], w)
            c3 = inward(value)
            value, tokens[2] = project([tokens[2]], w)
            c2 = inward(value)
            b2 = inner(project([tokens[2]], w, [(c3, 0, False)]))
            b1 = inner(project([tokens[3]], w, [(c2, 0, False)]))
            d1 = inward(project([tokens[1]], w, [(b2, 0, False)]), ((1, 0), (2, 3)))
            total, tokens[0] = project([tokens[0]], w, [(a1, 0, False), (d1, 0, False), (b1, 0, True)])
            keyval = total
        else:
            s1 = inward(project([tokens[3], tokens[2]], w))
            s2 = inner(project([tokens[2], tokens[3]], w, [(s1, 0, False)]))
            s3 = outer(project([tokens[1]], w, [(s2, 0, True)]))
            total = project([tokens[0]], w, [(s3, 0, False), (s2, seqlen, True)])
        result = attend(count, scalars, total, 0 if g else kv_width, GROUP_HEADS[g], keyval)
        pieces.append(swap(result, "pool", 1))
    return jnp.concatenate(pieces, axis=1)[None, None]


def gather_plan(states, lengths, gain, w_query, w_keyval):
    own = lax.axis_index("pool")
    count = lax.axis_size("mp")
    normed = normalize(states, lax.dynamic_index_in_dim(gain, own, 0, keepdims=False))
    tokens = lax.all_gather(normed, "mp", axis=2, tiled=True)[0, 0]
    query, keyval = (
        jnp.dot(
            tokens,
            lax.all_gather(
                lax.all_to_all(w[0], "mp", split_axis=1, concat_axis=0, tiled=True), "dp", axis=0, tiled=True
            ),
            preferred_element_type=F32,
        ).astype(BF16)
        for w in (w_query, w_keyval)
    )
    live = lax.dynamic_index_in_dim(lengths, own, 0, keepdims=False)
    scalars = jnp.stack([jnp.int32(0), live[0]])
    result = attend(count, scalars, query, 0, query.shape[1] // HD, keyval)
    return swap(result, "pool", 1)[None, None]


def on_device(states, lengths, gain, w_query, w_keyval):
    n = lax.axis_size("dp")
    heads = w_query.shape[2] // lax.axis_size("mp") // HD
    if n == 4 and heads == sum(GROUP_HEADS):
        return line_plan(states, lengths, gain, w_query, w_keyval)
    return gather_plan(states, lengths, gain, w_query, w_keyval)


def solution(mesh):
    in_specs = (
        P("pool", "dp", "mp", None),
        P(None, "dp"),
        P(),
        P("pool", ("dp", "mp"), None),
        P("pool", ("dp", "mp"), None),
    )
    out_specs = P("pool", "dp", None, "mp")
    return jax.shard_map(
        on_device, mesh=mesh, in_specs=in_specs, out_specs=out_specs, check_vma=False
    )
```

```python
import functools
import math

import jax
import jax.numpy as jnp
from jax import lax
from jax.experimental import pallas as pl
from jax.experimental.pallas import tpu as pltpu
from jax.sharding import PartitionSpec as P

HD = 128
F32 = jnp.float32
BF16 = jnp.bfloat16


def swap(value, axis, bits):
    return lax.ppermute(value, axis, [(i, i ^ bits) for i in range(lax.axis_size(axis))])


def normalize(rows, gain_row):
    values = rows.astype(F32)
    meansq = jnp.mean(values * values, axis=-1, keepdims=True)
    return (values * lax.rsqrt(meansq + 1e-05) * gain_row.astype(F32)).astype(BF16)


SMEM = pl.BlockSpec(memory_space=pltpu.SMEM)
NEAR = pl.BlockSpec(memory_space=pltpu.VMEM)
ANY = pl.BlockSpec(memory_space=pl.ANY)
ALONE = pltpu.CompilerParams(vmem_limit_bytes=62 << 20)


def limit(held):
    return pltpu.CompilerParams(vmem_limit_bytes=held + (2 << 20))


def cost(flops, moved, exps=0):
    return pl.CostEstimate(flops=flops, bytes_accessed=moved, transcendentals=exps)


def columns_copies(target, span, kv_width, q_width, w_query, w_keyval, out, sems):
    copies, at = [], 0
    if span.start < kv_width:
        at = kv_width - span.start
        cols = pl.ds(pl.multiple_of(target * kv_width + span.start, HD), at)
        copies.append(pltpu.make_async_copy(w_keyval.at[:, cols], out.at[:, :at], sems.at[0]))
    lo, width = max(span.start, kv_width) - kv_width, span.stop - span.start
    cols = pl.ds(pl.multiple_of(target * q_width + lo, HD), width - at)
    copies.append(pltpu.make_async_copy(w_query.at[:, cols], out.at[:, at:], sems.at[1]))
    return copies


class Cuts:
    def __init__(self, wanted, widths, depth):
        self.wanted, self.widths = wanted, widths
        shapes = [(depth, span.stop - span.start) for _, span in wanted]
        self.out_shape = [jax.ShapeDtypeStruct(shape, BF16) for shape in shapes]
        self.scratch = [pltpu.VMEM(shape, BF16) for shape in shapes]
        self.scratch += [pltpu.SemaphoreType.DMA((len(wanted), 2)), pltpu.SemaphoreType.DMA((len(wanted),))]
        self.moved = sum(4 * rows * cols for rows, cols in shapes)

    def start(self, w_query, w_keyval, outs, scratch):
        me = lax.axis_index("mp")
        held, sems, out_sems = scratch[:-2], scratch[-2], scratch[-1]
        self.inward = [
            columns_copies(me ^ bits, span, *self.widths, w_query, w_keyval, held[i], sems.at[i])
            for i, (bits, span) in enumerate(self.wanted)
        ]
        self.outward = [pltpu.make_async_copy(held[i], outs[i], out_sems.at[i]) for i in range(len(outs))]
        for copies in self.inward:
            for copy in copies:
                copy.start()

    def pass_on(self):
        for copies, out in zip(self.inward, self.outward):
            for copy in copies:
                copy.wait()
            out.start()

    def finish(self):
        for out in self.outward:
            out.wait()


def cut_kernel(cuts, w_query, w_keyval, *refs):
    count = len(cuts.wanted)
    cuts.start(w_query, w_keyval, refs[:count], refs[count:])
    cuts.pass_on()
    cuts.finish()


def cut(cuts, w_query, w_keyval):
    return pl.pallas_call(
        functools.partial(cut_kernel, cuts),
        out_shape=cuts.out_shape,
        in_specs=[ANY, ANY],
        out_specs=[ANY] * len(cuts.wanted),
        scratch_shapes=cuts.scratch,
        compiler_params=ALONE,
        cost_estimate=cost(0, cuts.moved),
        name="cut",
    )(w_query, w_keyval)


def stack_kernel(spans, *refs):
    me = lax.axis_index("mp")
    blocks, o_ref, sems = refs[:-2], refs[-2], refs[-1]
    copies = []
    for r, (ref, span) in enumerate(zip(blocks, spans)):
        depth = ref.shape[0]
        rows = pl.ds(pl.multiple_of((me ^ r) * depth, depth), depth)
        copies.append(pltpu.make_async_copy(ref.at[:, span], o_ref.at[rows, :], sems.at[r]))
    for copy in copies:
        copy.start()
    for copy in copies:
        copy.wait()


def stack_rows(span, shared, blocks):
    depth = shared[0].shape[0]
    width = span.stop - span.start
    spans = [span] * len(shared) + [slice(0, width)] * len(blocks)
    shape = (depth * len(spans), width)
    return pl.pallas_call(
        functools.partial(stack_kernel, spans),
        out_shape=jax.ShapeDtypeStruct(shape, BF16),
        in_specs=[ANY] * len(spans),
        out_specs=NEAR,
        scratch_shapes=[pltpu.SemaphoreType.DMA((len(spans),))],
        compiler_params=limit(2 * shape[0] * width),
        cost_estimate=cost(0, 4 * shape[0] * width),
        name="stack",
    )(*shared, *blocks)


def begin_kernel(chunk, n, cuts, x_ref, gain_ref, w_query, w_keyval, *refs):
    count = len(cuts.wanted)
    outs, cut_outs, refs = refs[:n], refs[n : n + count], refs[n + count :]
    x_held, gain_held, scaled, sems, gain_sem, out_sems = refs[:6]
    own, z = lax.axis_index("pool"), lax.axis_index("dp")
    depth = outs[0].shape[1]
    pieces = [slice(at, at + chunk) for at in range(0, x_ref.shape[0], chunk)]
    copies = [pltpu.make_async_copy(x_ref.at[rows, :], x_held.at[rows, :], sems.at[i]) for i, rows in enumerate(pieces)]
    gain_copy = pltpu.make_async_copy(gain_ref, gain_held, gain_sem)
    copies[0].start()
    gain_copy.start()
    for copy in copies[1:]:
        copy.start()
    cuts.start(w_query, w_keyval, cut_outs, refs[6:])
    gain_copy.wait()
    gain_row = jnp.where(own == 0, gain_held[0:1, :].astype(F32), gain_held[1:2, :].astype(F32))
    outward = []
    for i, rows in enumerate(pieces):
        copies[i].wait()
        values = x_held[rows, :].astype(F32)
        meansq = jnp.mean(values * values, axis=-1, keepdims=True)
        scaled[rows, :] = (values * lax.rsqrt(meansq + 1e-05) * gain_row).astype(BF16)
        for s, o_ref in enumerate(outs):
            cols = pl.ds(pl.multiple_of((z ^ s) * depth, depth), depth)
            out = pltpu.make_async_copy(scaled.at[rows, cols], o_ref.at[rows, :], out_sems.at[i, s])
            out.start()
            outward.append(out)
        if i == len(pieces) // 2:
            cuts.pass_on()
    for out in outward:
        out.wait()
    cuts.finish()


def begin(rows, gain, w_query, w_keyval, n, cuts):
    count, width = rows.shape
    chunk = min(16, count)
    outs = pl.pallas_call(
        functools.partial(begin_kernel, chunk, n, cuts),
        out_shape=[jax.ShapeDtypeStruct((count, width // n), BF16)] * n + cuts.out_shape,
        in_specs=[ANY] * 4,
        out_specs=[ANY] * (n + len(cuts.wanted)),
        scratch_shapes=[
            pltpu.VMEM(rows.shape, BF16),
            pltpu.VMEM(gain.shape, BF16),
            pltpu.VMEM(rows.shape, BF16),
            pltpu.SemaphoreType.DMA((count // chunk,)),
            pltpu.SemaphoreType.DMA,
            pltpu.SemaphoreType.DMA((count // chunk, n)),
        ]
        + cuts.scratch,
        compiler_params=ALONE,
        cost_estimate=cost(4 * count * width, 4 * count * width + cuts.moved),
        name="begin",
    )(rows, gain, w_query, w_keyval)
    return outs[:n], outs[n:]


def project_kernel(sizes, added, *refs):
    count = sum(sizes)
    blocks, w_ref, more, refs = refs[:count], refs[count], refs[count + 1 :][: len(added)], refs[count + 1 + len(added) :]
    o_ref = refs[0]
    seqlen = o_ref.shape[0] // len(sizes)
    z = lax.axis_index("dp")
    middle = (z == 1) | (z == 2)
    for t, size in enumerate(sizes):
        mine, blocks = blocks[:size], blocks[size:]
        if size == 1:
            tokens = mine[0][...]
        else:
            rows = mine[0].shape[0]
            for i, ref in enumerate(mine):
                refs[1][i * rows : (i + 1) * rows, :] = ref[...]
            tokens = refs[1][...]
        total = jnp.dot(tokens, w_ref[...], preferred_element_type=F32)
        for ref, (start, masked) in zip(more, added):
            part = ref[start + t * seqlen : start + (t + 1) * seqlen, :].astype(F32)
            total = total + (jnp.where(middle, part, 0.0) if masked else part)
        o_ref[t * seqlen : (t + 1) * seqlen, :] = total.astype(BF16)


def project(tokens, weights, added=()):
    join = isinstance(tokens[0], list)
    groups = tokens if join else [[array] for array in tokens]
    depth, width = weights.shape
    seqlen = sum(block.shape[0] for block in groups[0])
    flat = [block for group in groups for block in group]
    rows = seqlen * len(groups)
    out_shape = [jax.ShapeDtypeStruct((rows, width), BF16)]
    if join:
        out_shape.append(jax.ShapeDtypeStruct((seqlen, depth), BF16))
    out = pl.pallas_call(
        functools.partial(
            project_kernel, [len(group) for group in groups], [(start, masked) for _, start, masked in added]
        ),
        out_shape=out_shape,
        in_specs=[NEAR] * (len(flat) + 1 + len(added)),
        out_specs=[NEAR] * len(out_shape),
        compiler_params=limit(4 << 20),
        cost_estimate=cost(2 * rows * depth * width, 2 * rows * depth + 2 * depth * width + 2 * rows * width),
        name="project",
    )(*flat, weights, *[array for array, _, _ in added])
    return out if join else out[0]


def attend_kernel(count, heads, skip, scalars, q_ref, kv_ref, o_ref, keys, turned, values):
    me, length = scalars[0], scalars[1]
    seqlen = keys.shape[0]
    block = seqlen // count
    starts = [pl.multiple_of((b ^ me) * block, block) for b in range(count)]
    for b in range(count):
        keys[b * block : (b + 1) * block, :] = kv_ref[pl.ds(starts[b], block), :HD]
        values[b * block : (b + 1) * block, :] = kv_ref[pl.ds(starts[b], block), HD : 2 * HD]
    turned[...] = keys[...].T
    for b in range(count):
        reach = (b + 1) * block
        query = jnp.concatenate(
            [q_ref[pl.ds(starts[b], block), skip + h * HD : skip + (h + 1) * HD] for h in range(heads)], axis=0
        )
        scores = jnp.dot(query, turned[:, :reach], preferred_element_type=F32)
        places = b * block + lax.rem(lax.broadcasted_iota(jnp.int32, (heads * block, 1), 0), block)
        last = jnp.minimum(places, length - 1)
        allowed = lax.broadcasted_iota(jnp.int32, (heads * block, reach), 1) <= last
        scores = jnp.where(allowed, scores, jnp.float32(-1e30))
        scale = math.log2(math.e) / math.sqrt(HD)
        expo = jnp.exp2((scores - jnp.max(scores, axis=-1, keepdims=True)) * scale)
        result = jnp.dot(expo.astype(BF16), values[:reach, :], preferred_element_type=F32)
        result = result * (1.0 / jnp.sum(expo, axis=-1, keepdims=True))
        result = jnp.where(places < length, result, 0.0).astype(BF16)
        for h in range(heads):
            o_ref[b * block : reach, h * HD : (h + 1) * HD] = result[h * block : (h + 1) * block]


def attend(count, scalars, query, skip, heads, keyval):
    seqlen = keyval.shape[0]
    return pl.pallas_call(
        functools.partial(attend_kernel, count, heads, skip),
        out_shape=jax.ShapeDtypeStruct((seqlen, heads * HD), BF16),
        in_specs=[SMEM, NEAR, NEAR],
        out_specs=NEAR,
        scratch_shapes=[pltpu.VMEM(shape, BF16) for shape in ((seqlen, HD), (HD, seqlen), (seqlen, HD))],
        cost_estimate=cost(4 * seqlen * seqlen * HD * heads, 4 * seqlen * HD * heads, seqlen * seqlen * heads),
        compiler_params=limit(4 * seqlen * (query.shape[1] + seqlen * heads)),
        name="attend",
    )(scalars, query, keyval)


GROUP_HEADS = (2, 2, 2, 2)


def line_plan(states, lengths, gain, w_query, w_keyval):
    own = lax.axis_index("pool")
    n = lax.axis_size("dp")
    count = lax.axis_size("mp")
    me = lax.axis_index("mp")
    q_width = w_query.shape[2] // count
    kv_width = w_keyval.shape[2] // count
    w_query, w_keyval = w_query[0], w_keyval[0]

    spans, at = [], 0
    for g, heads in enumerate(GROUP_HEADS):
        to = at + heads * HD + (0 if g else kv_width)
        spans.append(slice(at, to))
        at = to

    widths = (kv_width, q_width)
    far = list(range(2, count))
    first = Cuts([(s, spans[0]) for s in far], widths, w_query.shape[0])
    normed, sent = begin(states[0, 0], gain, w_query, w_keyval, n, first)
    wanted = [(s, span) for span in spans[1:] for s in far] + [(bits, slice(0, at)) for bits in (0, 1)]
    *rest, mine, near = cut(Cuts(wanted, widths, w_query.shape[0]), w_query, w_keyval)
    sent = list(sent) + rest
    received = [[swap(sent[g * len(far) + i], "mp", s) for i, s in enumerate(far)] for g in range(len(spans))]
    near = swap(near, "mp", 1)
    weights = []
    for g, span in enumerate(spans):
        weights.append(stack_rows(span, [mine, near], received[g]))

    tokens = {}
    for s in range(n):
        piece = normed[s]
        if s:
            piece = swap(piece, "dp", s)
        blocks = {0: piece}
        bit = count // 2
        while bit:
            for have in list(blocks):
                blocks[have | bit] = swap(blocks[have], "mp", bit)
            bit //= 2
        tokens[s] = [blocks[j] for j in range(count)]

    def outer(value):
        return swap(value, "dp", 1)

    def inward(value, pairs=((0, 1), (3, 2))):
        return lax.ppermute(value, "dp", pairs)

    def inner(value):
        pairs = [(x * n + i, x * n + 3 - i) for x in range(2) for i in (1, 2)]
        pairs += [(x * n + i, (1 - x) * n + i) for x in range(2) for i in (0, 3)]
        return lax.ppermute(value, ("pool", "dp"), pairs)

    live = lax.dynamic_index_in_dim(lengths, own, 0, keepdims=False)
    scalars = jnp.stack([me.astype(jnp.int32), live[0]])
    seqlen = count * states.shape[2]
    pieces = []
    keyval = None
    for g, w in enumerate(weights):
        if g == 0:
            value, tokens[1] = project([tokens[1]], w)
            a1 = inward(value)
            value, tokens[3] = project([tokens[3]], w)
            c3 = inward(value)
            value, tokens[2] = project([tokens[2]], w)
            c2 = inward(value)
            b2 = inner(project([tokens[2]], w, [(c3, 0, False)]))
            b1 = inner(project([tokens[3]], w, [(c2, 0, False)]))
            d1 = inward(project([tokens[1]], w, [(b2, 0, False)]), ((1, 0), (2, 3)))
            total, tokens[0] = project([tokens[0]], w, [(a1, 0, False), (d1, 0, False), (b1, 0, True)])
            keyval = total
        else:
            s1 = inward(project([tokens[3], tokens[2]], w))
            value = project([tokens[2], tokens[3]], w, [(s1, 0, False)])
            s2 = inner(value)
            s3 = outer(project([tokens[1]], w, [(s2, 0, True)]))
            total = project([tokens[0]], w, [(s3, 0, False), (s2, seqlen, True)])
        result = attend(count, scalars, total, 0 if g else kv_width, GROUP_HEADS[g], keyval)
        pieces.append(swap(result, "pool", 1))
    return jnp.concatenate(pieces, axis=1)[None, None]


def gather_plan(states, lengths, gain, w_query, w_keyval):
    own = lax.axis_index("pool")
    count = lax.axis_size("mp")
    normed = normalize(states, lax.dynamic_index_in_dim(gain, own, 0, keepdims=False))
    tokens = lax.all_gather(normed, "mp", axis=2, tiled=True)[0, 0]
    query, keyval = (
        jnp.dot(
            tokens,
            lax.all_gather(
                lax.all_to_all(w[0], "mp", split_axis=1, concat_axis=0, tiled=True), "dp", axis=0, tiled=True
            ),
            preferred_element_type=F32,
        ).astype(BF16)
        for w in (w_query, w_keyval)
    )
    live = lax.dynamic_index_in_dim(lengths, own, 0, keepdims=False)
    scalars = jnp.stack([jnp.int32(0), live[0]])
    result = attend(count, scalars, query, 0, query.shape[1] // HD, keyval)
    return swap(result, "pool", 1)[None, None]


def on_device(states, lengths, gain, w_query, w_keyval):
    n = lax.axis_size("dp")
    heads = w_query.shape[2] // lax.axis_size("mp") // HD
    if n == 4 and heads == sum(GROUP_HEADS):
        return line_plan(states, lengths, gain, w_query, w_keyval)
    return gather_plan(states, lengths, gain, w_query, w_keyval)


def solution(mesh):
    in_specs = (
        P("pool", "dp", "mp", None),
        P(None, "dp"),
        P(),
        P("pool", ("dp", "mp"), None),
        P("pool", ("dp", "mp"), None),
    )
    out_specs = P("pool", "dp", None, "mp")
    return jax.shard_map(
        on_device, mesh=mesh, in_specs=in_specs, out_specs=out_specs, check_vma=False
    )
```
